32 devices in a mesh: dp: 2 (over core), seq: 16 (over z, y, x).
Axes of the slice: x: 2, y: 2, z: 4, core: 2. Of those that a mesh axis runs over, the one named last changes fastest.
Arguments:
- latent: bfloat16 [32, 1024, 1152], P(('dp', 'seq')), parts along dimension 0, may hold values from -6 to 6
- w_qkv_space: bfloat16 [1152, 1728], replicated, may hold values from -0.1875 to 0.1875
- w_out_space: bfloat16 [576, 1152], replicated, may hold values from -0.25 to 0.25
- w_qkv_time: bfloat16 [1152, 1728], replicated, may hold values from -0.1875 to 0.1875
- w_out_time: bfloat16 [576, 1152], replicated, may hold values from -0.25 to 0.25
- modulation: float32 [12, 1152], P('dp'), parts along dimension 0, may hold values from -1.5 to 5
Outputs:
- block_out: bfloat16 [32, 1024, 1152], P(('dp', 'seq')), parts along dimension 0
The draws below stay inside these ranges and needn't reach their ends.
There are 2 independent parts, one for each index of `dp`. The reference program is written for one: setup_inputs(seed, part) draws one part's arguments, and reference() takes and returns one part's arrays. A program takes and returns all parts, laid end to end along the dimension named above; an argument that names none is the same for every part. Nothing has to cross between parts.
All inputs are finite; a program needn't handle non-finite values.
Results may differ from the reference program's by a relative error of at most 0.02.
The reference program's roundings to bfloat16 on the way count: a program that leaves them out, or rounds other values in their place, can miss the bound.
Values may be sent and summed in bfloat16 or wider, within the bound.
A program may use at most 128 MiB of HBM per device.

```python
import jax
import jax.numpy as jnp
from jax import lax

D = 1152
HEADS = 8
HEAD_DIM = 72
S = 1024
FRAMES = 16


def draw_modulation(key, part):
    key_one = jax.random.fold_in(jax.random.fold_in(key, 17), 0)
    normal = jax.random.normal(key_one, (6, D), jnp.float32) * 0.5
    return jnp.clip(normal, -1.5, 1.5)


def level_of(rng, shape, cuts, smallest, largest):
    level, own = 1.0, jax.random.fold_in(rng, 6)
    for dim, shards_of in cuts:
        draws = jnp.exp(jax.random.uniform(jax.random.fold_in(own, dim), (shards_of,), jnp.float32, smallest / len(cuts), largest / len(cuts)))
        level = level * jnp.repeat(draws, shape[dim] // shards_of).reshape([-1 if axis == dim else 1 for axis in range(len(shape))])
    return level


def bell_draw(own_key, extent, scale, reach, shards=(), kind=jnp.bfloat16):
    array = scale * jax.random.normal(own_key, extent, jnp.float32)
    if shards:
        array = array * level_of(own_key, extent, shards, -0.22, 0.18)
    return jnp.clip(array, -reach, reach).astype(kind)


def setup_inputs(seed: int = 0, part: int = 0) -> dict:
    seeds = jax.random.split(jax.random.key(seed), 7)
    part_keys = jax.random.split(jax.random.fold_in(seeds[6], part), 7)
    latent = bell_draw(part_keys[0], (FRAMES, S, D), 1.0, 6.0, ((0, 16),))
    w_qkv_space = bell_draw(seeds[1], (D, 3 * HEADS * HEAD_DIM), D ** -0.5, 0.1875)
    w_out_space = bell_draw(seeds[2], (HEADS * HEAD_DIM, D), (HEADS * HEAD_DIM) ** -0.5, 0.25)
    w_qkv_time = bell_draw(seeds[3], (D, 3 * HEADS * HEAD_DIM), D ** -0.5, 0.1875)
    w_out_time = bell_draw(seeds[4], (HEADS * HEAD_DIM, D), (HEADS * HEAD_DIM) ** -0.5, 0.25)
    modulation = draw_modulation(jax.random.fold_in(jax.random.fold_in(seeds[6], part), 71), part)
    return {"latent": latent, "w_qkv_space": w_qkv_space, "w_out_space": w_out_space, "w_qkv_time": w_qkv_time, "w_out_time": w_out_time, "modulation": modulation}


EPS = 1e-06

def normalize(values):
    center = lax.optimization_barrier(jnp.mean(values, -1, keepdims=True))
    centred = values - center
    spread = lax.optimization_barrier(jnp.mean(centred * centred, -1, keepdims=True))
    return centred * lax.rsqrt(spread + EPS)

def modulated(latent, modulation, first):
    normed = normalize(latent.astype(jnp.float32))
    return (normed * (1.0 + modulation[first + 1]) + modulation[first]).astype(jnp.bfloat16)

def softmax_weights(scores, axis):
    top_score = lax.optimization_barrier(jnp.max(scores, axis, keepdims=True))
    expo = jnp.exp(scores - top_score)
    return (expo / lax.optimization_barrier(jnp.sum(expo, axis, keepdims=True))).astype(jnp.bfloat16)

def attend_space(frame_rows, w_qkv, w_out, modulation):
    tokens_here = frame_rows.shape[0]
    mixed = modulated(frame_rows, modulation, 0)
    triple = jnp.dot(mixed, w_qkv, preferred_element_type=jnp.float32).astype(jnp.bfloat16)
    triple = triple.reshape(tokens_here, 3, HEADS, HEAD_DIM).astype(jnp.float32)
    factor = 1.0 / math_sqrt(HEAD_DIM)
    scores = jnp.einsum('shd,thd->hst', triple[:, 0], triple[:, 1]) * factor
    weights = softmax_weights(scores, 2).astype(jnp.float32)
    outputs = jnp.einsum('hst,thd->shd', weights, triple[:, 2]).astype(jnp.bfloat16)
    delta = jnp.dot(outputs.reshape(tokens_here, HEADS * HEAD_DIM), w_out, preferred_element_type=jnp.float32)
    return (frame_rows.astype(jnp.float32) + modulation[2] * delta).astype(jnp.bfloat16)

def math_sqrt(value):
    return float(value) ** 0.5

def attend_time(queries, key_heads, value_heads):
    factor = 1.0 / math_sqrt(queries.shape[-1])
    scores = jnp.einsum('fphd,gphd->phfg', queries.astype(jnp.float32), key_heads.astype(jnp.float32)) * factor
    weights = softmax_weights(scores, 3).astype(jnp.float32)
    return jnp.einsum('phfg,gphd->fphd', weights, value_heads.astype(jnp.float32)).astype(jnp.bfloat16)

def reference(latent, w_qkv_space, w_out_space, w_qkv_time, w_out_time, modulation):
    after_space = lax.map(lambda one_frame: attend_space(one_frame, w_qkv_space, w_out_space, modulation), latent)
    frames, spatial, width = after_space.shape
    mixed = modulated(after_space, modulation, 3).reshape(frames * spatial, width)
    triple = jnp.dot(mixed, w_qkv_time, preferred_element_type=jnp.float32).astype(jnp.bfloat16)
    triple = triple.reshape(frames, spatial, 3, HEADS, HEAD_DIM)
    outputs = attend_time(triple[:, :, 0], triple[:, :, 1], triple[:, :, 2])
    delta = jnp.dot(outputs.reshape(frames * spatial, HEADS * HEAD_DIM), w_out_time, preferred_element_type=jnp.float32)
    result = after_space.astype(jnp.float32).reshape(frames * spatial, width) + modulation[5] * delta
    return result.astype(jnp.bfloat16).reshape(frames, spatial, width)
```

```python
import functools

import jax
import jax.numpy as jnp
from jax import lax
from jax.experimental import pallas as pl
from jax.experimental.pallas import tpu as pltpu
from jax.sharding import PartitionSpec as P

HEADS = 8
HEAD_DIM = 72
EPS = 1e-06
LANES = 128
TILE = 256
GROUP = 16
LOG2E = 1.4426950408889634
FAR = -1e30

f32, bf16 = jnp.float32, jnp.bfloat16


def modulated(rows, shift, scale):
    center = jnp.mean(rows, -1, keepdims=True)
    centred = rows - center
    spread = jnp.mean(centred * centred, -1, keepdims=True)
    return (centred * lax.rsqrt(spread + EPS) * (1.0 + scale) + shift).astype(bf16)


def windows(padded):
    out = []
    for head in range(HEADS):
        start = head * HEAD_DIM
        base = start // LANES * LANES
        wide = LANES if start + HEAD_DIM <= base + LANES else 2 * LANES
        base = min(base, padded - wide)
        out.append((base, wide, start - base))
    return out


def kernel(
    n, latent_hbm, wqs_hbm, wos_hbm, wqt_hbm, wot_hbm, mod, out_hbm,
    lat, wqs, wos, wqt, wot, q, k, v, attn, after, recv, bias, back_send, back_recv, out,
    load_sem, store_sem, send_sem, recv_sem, bsend_sem, brecv_sem,
):
    me = lax.axis_index("seq")
    tokens, width = lat.shape
    pos = tokens // n
    hd = HEADS * HEAD_DIM
    padded = q.shape[2]
    per = TILE // pos
    blocks = tokens // TILE
    half = blocks // 2
    groups = pos // GROUP
    keys = n * GROUP
    mine = me // per
    side, place = mine // half, mine % half
    factor = LOG2E / float(HEAD_DIM) ** 0.5

    def block_at(step):
        return (side + 1 - step // half) % 2 * half + (place + half - 1 - step % half) % half

    load_lat = pltpu.make_async_copy(latent_hbm.at[0], lat, load_sem.at[0])
    load_wqs = pltpu.make_async_copy(wqs_hbm, wqs, load_sem.at[1])
    load_wos = pltpu.make_async_copy(wos_hbm, wos, load_sem.at[2])
    load_wqt = pltpu.make_async_copy(wqt_hbm, wqt, load_sem.at[3])
    load_wot = pltpu.make_async_copy(wot_hbm, wot, load_sem.at[4])
    load_lat.start()
    load_wqs.start()

    barrier = pltpu.get_barrier_semaphore()

    def greet(i, _):
        pl.semaphore_signal(
            barrier, inc=1, device_id={"seq": (me + 1 + i) % n}, device_id_type=pl.DeviceIdType.MESH
        )
        return 0

    lax.fori_loop(0, n - 1, greet, 0)

    attn[...] = jnp.zeros_like(attn)
    v[:, :, hd:padded] = jnp.zeros((n, pos, padded - hd), bf16)
    row_at = lax.broadcasted_iota(jnp.int32, (keys, keys), 0) % GROUP
    col_at = lax.broadcasted_iota(jnp.int32, (keys, keys), 1) % GROUP
    bias[...] = jnp.where(row_at == col_at, 0.0, FAR).astype(f32)

    def project(block, mixed, weights):
        triple = jnp.dot(mixed, weights[...], preferred_element_type=f32)
        at = pl.ds(block * per, per)
        lead = hd - hd % LANES
        key_part = pltpu.roll(triple[:, lead : lead + padded], padded - (hd - lead), 1)
        q[at] = triple[:, :padded].astype(bf16).reshape(per, pos, padded)
        k[at] = key_part.astype(bf16).reshape(per, pos, padded)
        v[at, :, 0:hd] = triple[:, 2 * hd : 3 * hd].astype(bf16).reshape(per, pos, hd)

    def attend(queries, keys_of, values_of, add):
        for base, wide, offset in windows(padded):
            lane = lax.broadcasted_iota(jnp.int32, (1, wide), 1)
            inside = (lane >= offset) & (lane < offset + HEAD_DIM)
            only = inside.astype(f32).astype(bf16)
            scores = lax.dot_general(
                queries(base, wide) * only,
                keys_of(base, wide),
                (((1,), (1,)), ((), ())),
                preferred_element_type=f32,
            )
            if add is not None:
                scores = scores + add
            top = jnp.max(scores, -1, keepdims=True)
            expo = jnp.exp2((scores - top) * factor)
            total = jnp.sum(expo, -1, keepdims=True)
            mixture = jnp.dot(expo.astype(bf16), values_of(base, wide), preferred_element_type=f32)
            rows = mixture.shape[0]
            at = (slice(0, rows), slice(base, base + wide))
            attn[at] = jnp.where(inside, mixture * (1.0 / total), attn[at])

    load_lat.wait()
    load_wqs.wait()
    load_wos.start()
    load_wqt.start()
    load_wot.start()

    def space_project(block, _):
        rows = lat[pl.ds(pl.multiple_of(block * TILE, TILE), TILE), :].astype(f32)
        project(block, modulated(rows, mod[0:1], mod[1:2]), wqs)
        return 0

    lax.fori_loop(0, blocks, space_project, 0)
    load_wos.wait()
    pl.semaphore_wait(barrier, n - 1)

    def forward(to):
        rows = pl.ds(pl.multiple_of(to * pos, pos), pos)
        return pltpu.make_async_remote_copy(
            src_ref=after.at[rows, :],
            dst_ref=recv.at[me],
            send_sem=send_sem.at[to],
            recv_sem=recv_sem.at[me],
            device_id={"seq": to},
            device_id_type=pl.DeviceIdType.MESH,
        )

    def arrival(source):
        return pltpu.make_async_remote_copy(
            src_ref=after.at[pl.ds(0, pos), :],
            dst_ref=recv.at[source],
            send_sem=send_sem.at[source],
            recv_sem=recv_sem.at[source],
            device_id={"seq": source},
            device_id_type=pl.DeviceIdType.MESH,
        )

    def space_attend(step, _):
        block = block_at(step)
        at = pl.ds(block * per, per)
        attend(
            lambda base, wide: q[at, :, base : base + wide].reshape(TILE, wide),
            lambda base, wide: k[:, :, base : base + wide].reshape(tokens, wide),
            lambda base, wide: v[:, :, base : base + wide].reshape(tokens, wide),
            None,
        )
        rows = pl.ds(pl.multiple_of(block * TILE, TILE), TILE)
        delta = jnp.dot(attn[0:TILE, 0:hd].astype(bf16), wos[...], preferred_element_type=f32)
        after[rows, :] = (lat[rows, :].astype(f32) + mod[2:3] * delta).astype(bf16)
        for j in range(per):
            to = block * per + j

            @pl.when(to != me)
            def _():
                forward(to).start()

            @pl.when(to == me)
            def _():
                recv[me] = after[pl.ds(pl.multiple_of(to * pos, pos), pos), :]

        return 0

    lax.fori_loop(0, blocks, space_attend, 0)

    load_wqt.wait()
    load_wot.wait()

    def time_project(step, _):
        block = block_at(step)
        for j in range(per):
            source = block * per + j

            @pl.when(source != me)
            def _():
                arrival(source).wait_recv()

        rows = recv[pl.ds(block * per, per)].reshape(TILE, width).astype(f32)
        project(block, modulated(rows, mod[3:4], mod[4:5]), wqt)
        return 0

    lax.fori_loop(0, blocks, time_project, 0)

    def give_back(to, group):
        at = pl.ds(pl.multiple_of(group * GROUP, GROUP), GROUP)
        return pltpu.make_async_remote_copy(
            src_ref=back_send.at[to, at, :],
            dst_ref=back_recv.at[me, at, :],
            send_sem=bsend_sem.at[group, to],
            recv_sem=brecv_sem.at[group, me],
            device_id={"seq": to},
            device_id_type=pl.DeviceIdType.MESH,
        )

    def returned(source, group):
        at = pl.ds(pl.multiple_of(group * GROUP, GROUP), GROUP)
        return pltpu.make_async_remote_copy(
            src_ref=back_send.at[source, at, :],
            dst_ref=back_recv.at[source, at, :],
            send_sem=bsend_sem.at[group, source],
            recv_sem=brecv_sem.at[group, source],
            device_id={"seq": source},
            device_id_type=pl.DeviceIdType.MESH,
        )

    def time_attend(group, _):
        at = pl.ds(pl.multiple_of(group * GROUP, GROUP), GROUP)

        def rows_of(ref):
            return lambda base, wide: ref[:, at, base : base + wide].reshape(keys, wide)

        attend(rows_of(q), rows_of(k), rows_of(v), bias[...])
        back_send[:, at, :] = attn[0:keys, :].astype(bf16).reshape(n, GROUP, padded)
        back_recv[me, at, :] = back_send[me, at, :]

        def send(i, _):
            give_back((me + n // 2 + i) % n, group).start()
            return 0

        lax.fori_loop(0, n // 2, send, 0)
        lax.fori_loop(n // 2 + 1, n, send, 0)
        return 0

    lax.fori_loop(0, groups, time_attend, 0)

    def store(block):
        rows = pl.ds(pl.multiple_of(block * TILE, TILE), TILE)
        return pltpu.make_async_copy(out.at[rows, :], out_hbm.at[0, rows, :], store_sem.at[block])

    def finish(step, _):
        block = block_at(step)

        def wait_for(i, _):
            source = block * per + i // groups

            @pl.when(source != me)
            def _():
                returned(source, i % groups).wait_recv()

            return 0

        lax.fori_loop(0, per * groups, wait_for, 0)
        rows = pl.ds(pl.multiple_of(block * TILE, TILE), TILE)
        back = back_recv[pl.ds(block * per, per), :, 0:hd].reshape(TILE, hd)
        delta = jnp.dot(back, wot[...], preferred_element_type=f32)
        out[rows, :] = (after[rows, :].astype(f32) + mod[5:6] * delta).astype(bf16)
        store(block).start()
        return 0

    lax.fori_loop(0, blocks, finish, 0)

    def drain(i, _):
        to = (me + 1 + i) % n
        forward(to).wait_send()

        def drain_back(group, _):
            give_back(to, group).wait_send()
            return 0

        lax.fori_loop(0, groups, drain_back, 0)
        return 0

    lax.fori_loop(0, n - 1, drain, 0)

    def stored(block, _):
        store(block).wait()
        return 0

    lax.fori_loop(0, blocks, stored, 0)


def solution(mesh):
    n = mesh.shape["seq"]

    def step(latent, w_qkv_space, w_out_space, w_qkv_time, w_out_time, modulation):
        _, tokens, width = latent.shape
        pos = tokens // n
        hd = HEADS * HEAD_DIM
        padded = -(-hd // LANES) * LANES
        groups = pos // GROUP
        any_space = pl.BlockSpec(memory_space=pl.ANY)
        vmem = pltpu.VMEM
        dma = pltpu.SemaphoreType.DMA
        return pl.pallas_call(
            functools.partial(kernel, n),
            out_shape=jax.ShapeDtypeStruct(latent.shape, bf16),
            in_specs=[any_space] * 5 + [pl.BlockSpec(memory_space=pltpu.VMEM)],
            out_specs=any_space,
            scratch_shapes=[
                vmem((tokens, width), bf16),
                vmem(w_qkv_space.shape, bf16),
                vmem(w_out_space.shape, bf16),
                vmem(w_qkv_time.shape, bf16),
                vmem(w_out_time.shape, bf16),
                vmem((n, pos, padded), bf16),
                vmem((n, pos, padded), bf16),
                vmem((n, pos, padded), bf16),
                vmem((max(TILE, n * GROUP), padded), f32),
                vmem((tokens, width), bf16),
                vmem((n, pos, width), bf16),
                vmem((n * GROUP, n * GROUP), f32),
                vmem((n, pos, padded), bf16),
                vmem((n, pos, padded), bf16),
                vmem((tokens, width), bf16),
                dma((5,)),
                dma((tokens // TILE,)),
                dma((n,)),
                dma((n,)),
                dma((groups, n)),
                dma((groups, n)),
            ],
            compiler_params=pltpu.CompilerParams(
                collective_id=0, has_side_effects=True, vmem_limit_bytes=60 * 1024 * 1024
            ),
        )(latent, w_qkv_space, w_out_space, w_qkv_time, w_out_time, modulation)

    in_specs = (P(("dp", "seq"), None, None), P(), P(), P(), P(), P("dp", None))
    out_specs = P(("dp", "seq"), None, None)
    return jax.shard_map(step, mesh=mesh, in_specs=in_specs, out_specs=out_specs, check_vma=False)
```
